32 devices in a mesh: dp: 32 (over z, y, x, core).
Axes of the slice: x: 2, y: 2, z: 4, core: 2. Of those that a mesh axis runs over, the one named last changes fastest.
Arguments:
- token_ids: int32 [32768], P('dp'), may hold values from 0 to 31999, as said below
- tokens: bfloat16 [32768, 4096], P('dp'), may hold values from -64 to 64
- frozen_weight: bfloat16 [4096, 1024], replicated, may hold values from -0.09375 to 0.09375
- adapter_down: bfloat16 [4096, 128], replicated, may hold values from -0.09375 to 0.09375
- adapter_up: bfloat16 [128, 1024], replicated, may hold values from -1.5 to 1.5
- gate_weight: bfloat16 [4096, 8], replicated, may hold values from -1 to 1
- upstream: bfloat16 [32768, 1024], P('dp'), may hold values from -6 to 6
Outputs:
- projected: bfloat16 [32768, 1024], P('dp')
- input_grad: bfloat16 [32768, 4096], P('dp')
- clipped_down: float32 [4096, 128], replicated
- clipped_up: float32 [128, 1024], replicated
- clipped_gate: float32 [4096, 8], replicated
- load: float32 [8], replicated
- entropy: float32 [], replicated
The draws below stay inside these ranges and needn't reach their ends.
Inputs may be any that keep to these rules, and one draw needn't show every extreme that they name: `token_ids`: within each device's block of 1024 tokens the live tokens (id not 0) come first, 256 or more of them, and padding (id 0) fills the rest; the last block is wholly live.
All inputs are finite; a program needn't handle non-finite values.
Results may differ from the reference program's by a relative error of at most 0.0095.
Values sent between devices are 32-bit elements; how exact they have to be, the bound alone decides.
A program may use at most 192 MiB of HBM per device.

```python
import math
import jax
import jax.numpy as jnp
from jax import lax

D = 4096
DOUT = 1024
EXPERTS = 8
RANK = 16
VOCAB = 32000
TOK_DEV = 1024
TOKENS = 32768


def gate_table(key):
    return jax.random.normal(jax.random.fold_in(key, 7), (D, EXPERTS), jnp.float32) * (2.0 / math.sqrt(D))


def draw_gate_weight(key, part):
    return jnp.clip(gate_table(key), -1.0, 1.0).astype(jnp.bfloat16)


def draw_tokens(key, part):
    base_key = jax.random.fold_in(key, 11)
    noise = jax.random.normal(jax.random.fold_in(base_key, 1), (TOKENS, D), jnp.float32)
    scales = jnp.exp(jax.random.uniform(jax.random.fold_in(base_key, 2), (TOKENS, 1), jnp.float32, -math.log(2.0), math.log(2.0)))
    rows = noise * scales
    return jnp.clip(rows, -64.0, 64.0).astype(jnp.bfloat16)


def draw_token_ids(key, part):
    blocks = TOKENS // TOK_DEV
    block_ids = jnp.arange(blocks, dtype=jnp.int32)
    lowest = TOK_DEV // 4
    rising = (TOK_DEV - lowest) * block_ids // max(blocks - 1, 1)
    jitter = jax.random.randint(jax.random.fold_in(key, 21), (blocks,), 0, TOK_DEV // 8 + 1, dtype=jnp.int32)
    length = jnp.clip(lowest + rising - jitter, lowest, TOK_DEV)
    length = length.at[blocks - 1].set(TOK_DEV)
    position = jnp.arange(TOK_DEV, dtype=jnp.int32)
    alive = position[None, :] < length[:, None]
    values = jax.random.randint(jax.random.fold_in(key, 22), (blocks, TOK_DEV), 1, VOCAB, dtype=jnp.int32)
    return jnp.where(alive, values, 0).reshape(TOKENS).astype(jnp.int32)


def level_of(rng, dims, shards, smallest, high):
    level = 1.0
    for axis_at, shards_of in shards:
        steps = jax.random.uniform(jax.random.fold_in(jax.random.fold_in(rng, 6), axis_at), (shards_of,), jnp.float32, smallest / len(shards), high / len(shards))
        level = level * jnp.repeat(jnp.exp(steps), dims[axis_at] // shards_of).reshape((-1,) + (1,) * (len(dims) - 1 - axis_at))
    return level


def normal_values(stream_key, extent, scale, most, cuts=(), kind=jnp.bfloat16):
    values = jax.random.normal(stream_key, extent, jnp.float32) * scale
    if len(cuts) > 0:
        values = level_of(stream_key, extent, cuts, -0.22, 0.18) * values
    return jnp.clip(values, min=-most, max=most).astype(kind)


def setup_inputs(seed: int = 0) -> dict:
    streams_of = jax.random.split(jax.random.key(seed), 8)
    token_ids = draw_token_ids(jax.random.fold_in(streams_of[7], 71), 0)
    tokens = draw_tokens(jax.random.fold_in(streams_of[7], 71), 0)
    frozen_weight = normal_values(streams_of[2], (D, DOUT), D ** -0.5, 0.09375)
    adapter_down = normal_values(streams_of[3], (D, EXPERTS * RANK), D ** -0.5, 0.09375)
    adapter_up = normal_values(streams_of[4], (EXPERTS * RANK, DOUT), RANK ** -0.5, 1.5)
    gate_weight = draw_gate_weight(jax.random.fold_in(streams_of[7], 71), 0)
    upstream = normal_values(streams_of[6], (TOKENS, DOUT), 1.0, 6.0, ((0, 32),))
    return dict(token_ids=token_ids, tokens=tokens, frozen_weight=frozen_weight, adapter_down=adapter_down, adapter_up=adapter_up, gate_weight=gate_weight, upstream=upstream)


def reference(token_ids, tokens, frozen_weight, adapter_down, adapter_up, gate_weight, upstream):
    live = (token_ids != 0).astype(jnp.float32)
    base = jnp.dot(tokens, frozen_weight, preferred_element_type=jnp.float32)
    logits = jnp.dot(tokens, gate_weight, preferred_element_type=jnp.float32)
    prob = jax.nn.softmax(logits, axis=1)
    logp = jax.nn.log_softmax(logits, axis=1)
    low = jnp.dot(tokens, adapter_down, preferred_element_type=jnp.float32).astype(jnp.bfloat16)
    spread = jnp.repeat(prob, RANK, axis=1)
    weighted = (low.astype(jnp.float32) * spread).astype(jnp.bfloat16)
    projected = (base + 2.0 * jnp.dot(weighted, adapter_up, preferred_element_type=jnp.float32)).astype(jnp.bfloat16)
    masked = upstream * live.astype(jnp.bfloat16)[:, None]
    grad_up = 2.0 * jnp.dot(weighted.T, masked, preferred_element_type=jnp.float32)
    back = jnp.dot(masked, adapter_up.T, preferred_element_type=jnp.float32)
    gate_task = 2.0 * lax.optimization_barrier(jnp.sum((low.astype(jnp.float32) * back).reshape(-1, EXPERTS, RANK), axis=2))
    low_grad = (2.0 * spread * back).astype(jnp.bfloat16)
    grad_down = jnp.dot(tokens.T, low_grad, preferred_element_type=jnp.float32)
    ent_tok = -lax.optimization_barrier(jnp.sum(prob * logp, axis=1))
    load_sum = lax.optimization_barrier(jnp.sum(live[:, None] * prob, axis=0))
    ent_sum = jnp.sum(live * ent_tok)
    live_sum = jnp.sum(live)

    def jac(v):
        return prob * (v - lax.optimization_barrier(jnp.sum(prob * v, axis=1, keepdims=True)))
    gate_z = jac(gate_task) + 50.0 * live[:, None] * prob * (logp + ent_tok[:, None])
    gate_z = gate_z + 2.0 * EXPERTS * 100.0 / live_sum * live[:, None] * jac(load_sum[None, :])
    grad_gate = jnp.dot(tokens.astype(jnp.float32).T, gate_z, precision=lax.Precision.HIGHEST)
    input_grad = jnp.dot(masked, frozen_weight.T, preferred_element_type=jnp.float32)
    input_grad = input_grad + jnp.dot(low_grad, adapter_down.T, preferred_element_type=jnp.float32)
    input_grad = input_grad + jnp.dot(gate_z, gate_weight.astype(jnp.float32).T, precision=lax.Precision.HIGHEST)
    total = jnp.sum(grad_down * grad_down) + jnp.sum(grad_up * grad_up) + jnp.sum(grad_gate * grad_gate)
    count = D * EXPERTS * RANK + EXPERTS * RANK * DOUT + D * EXPERTS
    clip = jnp.minimum(1.0, math.sqrt(count) / jnp.sqrt(total))
    return (projected, input_grad.astype(jnp.bfloat16), grad_down * clip, grad_up * clip, grad_gate * clip, load_sum / live_sum, ent_sum / live_sum)
```

```python
import functools
import math

import jax
import jax.numpy as jnp
from jax import lax
from jax.experimental import pallas as pl
from jax.experimental.pallas import tpu as pltpu
from jax.sharding import PartitionSpec as P

MESH = pl.DeviceIdType.MESH
F32 = jnp.float32
BF16 = jnp.bfloat16


def nn(a, b):
    return jnp.dot(a, b, preferred_element_type=F32)


def nt(a, b):
    return lax.dot_general(a, b, (((1,), (1,)), ((), ())), preferred_element_type=F32)


def split(value):
    upper = value.astype(BF16)
    return upper, (value - upper.astype(F32)).astype(BF16)


def kernel(
    n, experts, orders, seg,
    ids, tok_hbm, fw_hbm, down_hbm, up_hbm, gate, ups_hbm,
    proj_hbm, ing_hbm, gd_out, gu_out, gg_out, st_out,
    tok, fw, wcat, up, ups, proj, ing, prob_s, plain_s, weighted_s, wt_s, lhs, lhs_t,
    acc, rbuf, gbuf, st_recv, st_send,
    in_sem, out_sem, st_ssem, st_rsem, rs_ssem, rs_rsem, ag_ssem, ag_rsem,
):
    me = lax.axis_index("dp")
    rows, width = tok.shape
    ranks, outputs = up.shape
    rank = ranks // experts
    step = min(256, rows)
    chunks = rows // step
    nbits = len(orders[0])
    streams = len(orders)

    loads = {}

    def load(name, index, src, dst):
        loads[name] = pltpu.make_async_copy(src, dst, in_sem.at[index])
        loads[name].start()

    load("down", 2, down_hbm, wcat.at[:, pl.ds(0, ranks)])
    load("up", 0, up_hbm, up)
    load("ups", 1, ups_hbm, ups)
    for c in range(chunks):
        part = pl.ds(c * step, step)
        load(("tok", c), 4 + c, tok_hbm.at[part, :], tok.at[part, :])
    load("fw", 3, fw_hbm, fw)

    barrier = pltpu.get_barrier_semaphore()
    for k in range(1, n):
        pl.semaphore_signal(
            barrier, inc=1, device_id=(lax.rem(me + k, n),), device_id_type=MESH
        )

    loads["down"].wait()
    erow = lax.broadcasted_iota(jnp.int32, (experts, ranks), 0)
    ecol = lax.broadcasted_iota(jnp.int32, (experts, ranks), 1) // rank
    expand = (erow == ecol).astype(F32)
    for c in range(0, width, 512):
        wcat[pl.ds(c, 512), pl.ds(ranks, ranks)] = nn(
            gate[:, pl.ds(c, 512)].astype(F32).T.astype(BF16), expand.astype(BF16)
        ).astype(BF16)
    brow = lax.broadcasted_iota(jnp.int32, (ranks, ranks), 0) // rank
    bcol = lax.broadcasted_iota(jnp.int32, (ranks, ranks), 1) // rank
    block = (brow == bcol).astype(F32).astype(BF16)
    count = jnp.sum((ids[...] != 0).astype(F32), axis=(0, 1), keepdims=True)

    def alive(c):
        at = lax.broadcasted_iota(jnp.int32, (step, 1), 0) + c * step
        return (at.astype(F32) < count).astype(F32)

    def lane_mean(value):
        return jnp.sum(value, axis=1, keepdims=True) * (1.0 / rank)

    loads["up"].wait()
    loads["ups"].wait()
    load_sum = jnp.zeros((1, ranks), F32)
    ent_sum = jnp.zeros((1, 1), F32)
    for c in range(chunks):
        part = pl.ds(c * step, step)
        live = alive(c)
        masked = ups[part, :] * live.astype(BF16)
        ups[part, :] = masked
        back = nt(masked, up[...])
        loads[("tok", c)].wait()
        both = nn(tok[part, :], wcat[...])
        low = both[:, :ranks].astype(BF16).astype(F32)
        logits = both[:, ranks:]
        shifted = logits - jnp.max(logits, axis=1, keepdims=True)
        ex = jnp.exp(shifted)
        total = lane_mean(ex)
        prob = ex / total
        logp = shifted - jnp.log(total)
        ent = -lane_mean(prob * logp)
        load_sum += jnp.sum(live * prob, axis=0, keepdims=True)
        ent_sum += jnp.sum(live * ent, axis=0, keepdims=True)
        weighted = low * prob
        weighted_s[part, :] = weighted.astype(BF16)
        wt_s[:, part] = weighted.T.astype(BF16)
        upper, lower = split(low * back)
        task = 2.0 * (nn(upper, block) + nn(lower, block))
        plain_s[part, :] = prob * (task - lane_mean(prob * task)) + 50.0 * live * prob * (logp + ent)
        prob_s[part, :] = prob
        low_grad = 2.0 * prob * back
        lhs[part, pl.ds(0, ranks)] = low_grad.astype(BF16)
        lhs_t[pl.ds(0, ranks), part] = low_grad.T.astype(BF16)

    srow = lax.broadcasted_iota(jnp.int32, (8, ranks), 0)
    st_send[...] = jnp.where(srow == 0, load_sum, jnp.where(srow == 1, ent_sum, count))
    pl.semaphore_wait(barrier, n - 1)
    stats = []
    for k in range(1, n):
        copy = pltpu.make_async_remote_copy(
            src_ref=st_send,
            dst_ref=st_recv.at[k - 1],
            send_sem=st_ssem.at[k - 1],
            recv_sem=st_rsem.at[k - 1],
            device_id=(lax.rem(me + k, n),),
            device_id_type=MESH,
        )
        copy.start()
        stats.append(copy)

    for j in range(outputs // 128):
        part = pl.ds(j * 128, 128)
        if j % 2 == 0:
            two = 2.0 * nn(wt_s[...], ups[:, pl.ds(j * 128, 256)])
        acc[pl.ds(width + j * 128, 128), :] = two[:, (j % 2) * 128:(j % 2) * 128 + 128]

    stores = []

    def store(src, dst):
        copy = pltpu.make_async_copy(src, dst, out_sem.at[len(stores)])
        copy.start()
        stores.append(copy)

    def do_proj(j):
        part = pl.ds(j * 256, 256)
        proj[:, part] = (
            nn(tok[...], fw[:, part]) + 2.0 * nn(weighted_s[...], up[:, part])
        ).astype(BF16)
        store(proj.at[:, part], proj_hbm.at[:, part])

    def do_ing(j):
        part = pl.ds(j * 512, 512)
        ing[:, part] = (
            nt(ups[...], fw[part, :]) + nt(lhs[...], wcat[part, :])
        ).astype(BF16)
        store(ing.at[:, part], ing_hbm.at[:, part])

    loads["fw"].wait()
    do_proj(0)

    for copy in stats:
        copy.wait()
    everyone = st_send[...] + jnp.sum(st_recv[...], axis=0)
    load_all = everyone[0:1, :]
    live_all = everyone[2:3, 0:1]
    st_out[...] = everyone / live_all
    lane = lax.rem(lax.broadcasted_iota(jnp.int32, (step, ranks), 1), rank)
    for c in range(chunks):
        part = pl.ds(c * step, step)
        prob = prob_s[part, :]
        gate_z = plain_s[part, :] + (2.0 * experts * 100.0 / live_all) * alive(c) * prob * (
            load_all - lane_mean(prob * load_all)
        )
        upper, lower = split(gate_z)
        picked = jnp.where(
            lane == 0, upper.astype(F32), jnp.where(lane == 1, lower.astype(F32), 0.0)
        )
        lhs[part, pl.ds(ranks, ranks)] = picked.astype(BF16)
        lhs_t[pl.ds(ranks, ranks), part] = picked.T.astype(BF16)

    gate_at = width + outputs
    for c in range(0, width, 512):
        out = nn(lhs_t[...], tok[:, pl.ds(c, 512)])
        gates = jnp.sum(out[ranks:, :].reshape(experts, rank, 512), axis=1)
        for j in range(4):
            acc[pl.ds(c + j * 128, 128), :] = out[:ranks, j * 128:(j + 1) * 128]
            acc[pl.ds(gate_at + (c // 128 + j) * experts, experts), :] = gates[
                :, j * 128:(j + 1) * 128
            ]
    used = gate_at + width // 128 * experts
    if streams * seg > used:
        acc[pl.ds(used, streams * seg - used), :] = jnp.zeros((streams * seg - used, 128), F32)

    bases = [[s * seg] for s in range(streams)]
    flying = []

    def side(bit):
        return lax.rem(me // (1 << bit), 2)

    def scatter_start(k):
        half = seg >> (k + 1)
        for s in range(streams):
            bit = orders[s][k]
            beta = side(bit)
            away = pl.multiple_of(bases[s][k] + (1 - beta) * half, 8)
            keep = pl.multiple_of(bases[s][k] + beta * half, 8)
            bases[s].append(keep)
            copy = pltpu.make_async_remote_copy(
                src_ref=acc.at[pl.ds(away, half), :],
                dst_ref=rbuf.at[pl.ds(s * seg + seg - 2 * half, half), :],
                send_sem=rs_ssem.at[s * nbits + k],
                recv_sem=rs_rsem.at[s * nbits + k],
                device_id=(me + (1 - 2 * beta) * (1 << bit),),
                device_id_type=MESH,
            )
            copy.start()
            flying.append(copy)

    def scatter_finish(k):
        half = seg >> (k + 1)
        for s in range(streams):
            flying.pop(0).wait()
            keep = pl.ds(bases[s][k + 1], half)
            target = gbuf if k == nbits - 1 else acc
            target[keep, :] = acc[keep, :] + rbuf[pl.ds(s * seg + seg - 2 * half, half), :]

    def gather_start(k):
        half = seg >> (k + 1)
        for s in range(streams):
            bit = orders[s][k]
            part = pl.ds(bases[s][k + 1], half)
            copy = pltpu.make_async_remote_copy(
                src_ref=gbuf.at[part, :],
                dst_ref=gbuf.at[part, :],
                send_sem=ag_ssem.at[s * nbits + k],
                recv_sem=ag_rsem.at[s * nbits + k],
                device_id=(me + (1 - 2 * side(bit)) * (1 << bit),),
                device_id_type=MESH,
            )
            copy.start()
            flying.append(copy)

    def gather_finish(k):
        for s in range(streams):
            flying.pop(0).wait()

    work = [functools.partial(do_proj, j) for j in range(1, outputs // 256)]
    work += [functools.partial(do_ing, j) for j in range(width // 512)]
    rounds = 2 * nbits
    for r in range(rounds):
        k = r if r < nbits else rounds - 1 - r
        if r < nbits:
            scatter_start(k)
        else:
            gather_start(k)
        todo = -(-len(work) // (rounds - r))
        for _ in range(min(todo, len(work))):
            work.pop(0)()
        if r < nbits:
            scatter_finish(k)
        else:
            gather_finish(k)

    squares = jnp.zeros((8, 128), F32)
    for c in range(0, used, 128):
        piece = gbuf[pl.ds(c, 128), :]
        squares += jnp.sum((piece * piece).reshape(16, 8, 128), axis=0)
    norm = jnp.sqrt(jnp.sum(squares, axis=(0, 1), keepdims=True))
    limit = math.sqrt(width * ranks + ranks * outputs + width * experts)
    factor = jnp.minimum(1.0, limit / norm)
    for c in range(0, width, 128):
        gd_out[pl.ds(c, 128), :] = gbuf[pl.ds(c, 128), :].T * factor
        gg_out[:, pl.ds(c, 128)] = (
            gbuf[pl.ds(gate_at + c // 128 * experts, experts), :] * factor
        )
    for c in range(0, outputs, 128):
        gu_out[:, pl.ds(c, 128)] = gbuf[pl.ds(width + c, 128), :] * factor
    for copy in stores:
        copy.wait()


def on_device(n, token_ids, tokens, frozen_weight, adapter_down, adapter_up, gate_weight, upstream):
    rows, width = tokens.shape
    experts = gate_weight.shape[1]
    ranks = adapter_down.shape[1]
    rank = ranks // experts
    outputs = frozen_weight.shape[1]
    nbits = n.bit_length() - 1
    head = list(range(1, nbits - 1))
    streams = min(3, len(head))
    orders = [[0] + head[s:] + head[:s] + [nbits - 1] for s in range(streams)]
    used = width + outputs + width // 128 * experts
    unit = 8 * n
    seg = -(-used // (streams * unit)) * unit
    chunks = rows // min(256, rows)
    hbm = pl.BlockSpec(memory_space=pl.ANY)
    vmem = pl.BlockSpec(memory_space=pltpu.VMEM)
    dma = pltpu.SemaphoreType.DMA
    out = pl.pallas_call(
        functools.partial(kernel, n, experts, orders, seg),
        out_shape=(
            jax.ShapeDtypeStruct((rows, outputs), BF16),
            jax.ShapeDtypeStruct((rows, width), BF16),
            jax.ShapeDtypeStruct((width, ranks), F32),
            jax.ShapeDtypeStruct((ranks, outputs), F32),
            jax.ShapeDtypeStruct((experts, width), F32),
            jax.ShapeDtypeStruct((8, ranks), F32),
        ),
        in_specs=[vmem, hbm, hbm, hbm, hbm, vmem, hbm],
        out_specs=(hbm, hbm, vmem, vmem, vmem, vmem),
        scratch_shapes=[
            pltpu.VMEM((rows, width), BF16),
            pltpu.VMEM((width, outputs), BF16),
            pltpu.VMEM((width, 2 * ranks), BF16),
            pltpu.VMEM((ranks, outputs), BF16),
            pltpu.VMEM((rows, outputs), BF16),
            pltpu.VMEM((rows, outputs), BF16),
            pltpu.VMEM((rows, width), BF16),
            pltpu.VMEM((rows, ranks), F32),
            pltpu.VMEM((rows, ranks), F32),
            pltpu.VMEM((rows, ranks), BF16),
            pltpu.VMEM((ranks, rows), BF16),
            pltpu.VMEM((rows, 2 * ranks), BF16),
            pltpu.VMEM((2 * ranks, rows), BF16),
            pltpu.VMEM((streams * seg, 128), F32),
            pltpu.VMEM((streams * seg, 128), F32),
            pltpu.VMEM((streams * seg, 128), F32),
            pltpu.VMEM((n - 1, 8, ranks), F32),
            pltpu.VMEM((8, ranks), F32),
            dma((4 + chunks,)),
            dma((outputs // 256 + width // 512,)),
            dma((n - 1,)),
            dma((n - 1,)),
            dma((streams * nbits,)),
            dma((streams * nbits,)),
            dma((streams * nbits,)),
            dma((streams * nbits,)),
        ],
        compiler_params=pltpu.CompilerParams(
            collective_id=0, vmem_limit_bytes=60 * 1024 * 1024
        ),
    )(
        token_ids.reshape(rows // 128, 128), tokens, frozen_weight, adapter_down, adapter_up,
        gate_weight.T, upstream,
    )
    proj, ing, down, up, gate, stats = out
    return proj, ing, down, up, gate.T, stats[0, ::rank], stats[1, 0]


def solution(mesh):
    placed = (P("dp"), P("dp", None), P(), P(), P(), P(), P("dp", None))
    return jax.shard_map(
        functools.partial(on_device, mesh.shape["dp"]),
        mesh=mesh,
        in_specs=placed,
        out_specs=(P("dp", None), P("dp", None), P(), P(), P(), P(), P()),
        check_vma=False,
    )
```

```python
import functools
import math

import jax
import jax.numpy as jnp
from jax import lax
from jax.experimental import pallas as pl
from jax.experimental.pallas import tpu as pltpu
from jax.sharding import PartitionSpec as P

MESH = pl.DeviceIdType.MESH
F32 = jnp.float32
BF16 = jnp.bfloat16


def nn(a, b):
    return jnp.dot(a, b, preferred_element_type=F32)


def nt(a, b):
    return lax.dot_general(a, b, (((1,), (1,)), ((), ())), preferred_element_type=F32)


def split(value):
    upper = value.astype(BF16)
    return upper, (value - upper.astype(F32)).astype(BF16)


def kernel(
    n, experts, orders, segs,
    ids, tok_hbm, fw_hbm, down_hbm, up_hbm, gate, ups_hbm,
    proj, ing, gd_out, gu_out, gg_out, st_out,
    tok, fw, wcat, up, ups, prob_s, plain_s, weighted_s, wt_s, lhs, lhs_t,
    acc, rbuf, gbuf, st_recv, st_send,
    in_sem, st_ssem, st_rsem, rs_ssem, rs_rsem, ag_ssem, ag_rsem,
):
    me = lax.axis_index("dp")
    rows, width = tok.shape
    ranks, outputs = up.shape
    rank = ranks // experts
    step = min(256, rows)
    chunks = rows // step
    nbits = len(orders[0])
    streams = len(orders)

    loads = {}

    def load(name, index, src, dst):
        loads[name] = pltpu.make_async_copy(src, dst, in_sem.at[index])
        loads[name].start()

    load("down", 2, down_hbm, wcat.at[:, pl.ds(0, ranks)])
    load("up", 0, up_hbm, up)
    load("ups", 1, ups_hbm, ups)
    for c in range(chunks):
        part = pl.ds(c * step, step)
        load(("tok", c), 4 + c, tok_hbm.at[part, :], tok.at[part, :])
    load("fw", 3, fw_hbm, fw)

    barrier = pltpu.get_barrier_semaphore()
    for k in range(1, n):
        pl.semaphore_signal(
            barrier, inc=1, device_id=(lax.rem(me + k, n),), device_id_type=MESH
        )

    loads["down"].wait()
    erow = lax.broadcasted_iota(jnp.int32, (experts, ranks), 0)
    ecol = lax.broadcasted_iota(jnp.int32, (experts, ranks), 1) // rank
    expand = (erow == ecol).astype(F32)
    for c in range(0, width, 512):
        wcat[pl.ds(c, 512), pl.ds(ranks, ranks)] = nn(
            gate[:, pl.ds(c, 512)].astype(F32).T.astype(BF16), expand.astype(BF16)
        ).astype(BF16)
    brow = lax.broadcasted_iota(jnp.int32, (ranks, ranks), 0) // rank
    bcol = lax.broadcasted_iota(jnp.int32, (ranks, ranks), 1) // rank
    block = (brow == bcol).astype(F32).astype(BF16)
    count = jnp.sum((ids[...] != 0).astype(F32), axis=(0, 1), keepdims=True)

    def alive(c):
        at = lax.broadcasted_iota(jnp.int32, (step, 1), 0) + c * step
        return (at.astype(F32) < count).astype(F32)

    def lane_mean(value):
        return jnp.sum(value, axis=1, keepdims=True) * (1.0 / rank)

    loads["up"].wait()
    loads["ups"].wait()
    load_sum = jnp.zeros((1, ranks), F32)
    ent_sum = jnp.zeros((1, 1), F32)
    for c in range(chunks):
        part = pl.ds(c * step, step)
        live = alive(c)
        masked = ups[part, :] * live.astype(BF16)
        ups[part, :] = masked
        back = nt(masked, up[...])
        loads[("tok", c)].wait()
        both = nn(tok[part, :], wcat[...])
        low = both[:, :ranks].astype(BF16).astype(F32)
        logits = both[:, ranks:]
        shifted = logits - jnp.max(logits, axis=1, keepdims=True)
        ex = jnp.exp(shifted)
        total = lane_mean(ex)
        prob = ex / total
        logp = shifted - jnp.log(total)
        ent = -lane_mean(prob * logp)
        load_sum += jnp.sum(live * prob, axis=0, keepdims=True)
        ent_sum += jnp.sum(live * ent, axis=0, keepdims=True)
        weighted = low * prob
        weighted_s[part, :] = weighted.astype(BF16)
        wt_s[:, part] = weighted.T.astype(BF16)
        upper, lower = split(low * back)
        task = 2.0 * (nn(upper, block) + nn(lower, block))
        plain_s[part, :] = prob * (task - lane_mean(prob * task)) + 50.0 * live * prob * (logp + ent)
        prob_s[part, :] = prob
        low_grad = 2.0 * prob * back
        lhs[part, pl.ds(0, ranks)] = low_grad.astype(BF16)
        lhs_t[pl.ds(0, ranks), part] = low_grad.T.astype(BF16)

    srow = lax.broadcasted_iota(jnp.int32, (8, ranks), 0)
    st_send[...] = jnp.where(srow == 0, load_sum, jnp.where(srow == 1, ent_sum, count))
    pl.semaphore_wait(barrier, n - 1)
    stats = []
    for k in range(1, n):
        copy = pltpu.make_async_remote_copy(
            src_ref=st_send,
            dst_ref=st_recv.at[k - 1],
            send_sem=st_ssem.at[k - 1],
            recv_sem=st_rsem.at[k - 1],
            device_id=(lax.rem(me + k, n),),
            device_id_type=MESH,
        )
        copy.start()
        stats.append(copy)

    for j in range(outputs // 128):
        part = pl.ds(j * 128, 128)
        if j % 2 == 0:
            two = 2.0 * nn(wt_s[...], ups[:, pl.ds(j * 128, 256)])
        acc[pl.ds(width + j * 128, 128), :] = two[:, (j % 2) * 128:(j % 2) * 128 + 128]

    def do_proj(j):
        part = pl.ds(j * 256, 256)
        proj[:, part] = (
            nn(tok[...], fw[:, part]) + 2.0 * nn(weighted_s[...], up[:, part])
        ).astype(BF16)

    def do_ing(j):
        part = pl.ds(j * 512, 512)
        ing[:, part] = (
            nt(ups[...], fw[part, :]) + nt(lhs[...], wcat[part, :])
        ).astype(BF16)

    loads["fw"].wait()
    do_proj(0)

    for copy in stats:
        copy.wait()
    everyone = st_send[...] + jnp.sum(st_recv[...], axis=0)
    load_all = everyone[0:1, :]
    live_all = everyone[2:3, 0:1]
    st_out[...] = everyone / live_all
    lane = lax.rem(lax.broadcasted_iota(jnp.int32, (step, ranks), 1), rank)
    for c in range(chunks):
        part = pl.ds(c * step, step)
        prob = prob_s[part, :]
        gate_z = plain_s[part, :] + (2.0 * experts * 100.0 / live_all) * alive(c) * prob * (
            load_all - lane_mean(prob * load_all)
        )
        upper, lower = split(gate_z)
        picked = jnp.where(
            lane == 0, upper.astype(F32), jnp.where(lane == 1, lower.astype(F32), 0.0)
        )
        lhs[part, pl.ds(ranks, ranks)] = picked.astype(BF16)
        lhs_t[pl.ds(ranks, ranks), part] = picked.T.astype(BF16)

    gate_at = width + outputs
    for c in range(0, width, 512):
        out = nn(lhs_t[...], tok[:, pl.ds(c, 512)])
        gates = jnp.sum(out[ranks:, :].reshape(experts, rank, 512), axis=1)
        for j in range(4):
            acc[pl.ds(c + j * 128, 128), :] = out[:ranks, j * 128:(j + 1) * 128]
            acc[pl.ds(gate_at + (c // 128 + j) * experts, experts), :] = gates[
                :, j * 128:(j + 1) * 128
            ]
    used = gate_at + width // 128 * experts
    held = acc.shape[0]
    if held > used:
        acc[pl.ds(used, held - used), :] = jnp.zeros((held - used, 128), F32)

    starts = [sum(segs[:s]) for s in range(streams)]
    bases = [[at] for at in starts]
    flying = {}

    def side(bit):
        return lax.rem(me // (1 << bit), 2)

    def scatter_start(group, k):
        for s in group:
            half = segs[s] >> (k + 1)
            bit = orders[s][k]
            beta = side(bit)
            away = pl.multiple_of(bases[s][k] + (1 - beta) * half, 8)
            keep = pl.multiple_of(bases[s][k] + beta * half, 8)
            bases[s].append(keep)
            copy = pltpu.make_async_remote_copy(
                src_ref=acc.at[pl.ds(away, half), :],
                dst_ref=rbuf.at[pl.ds(starts[s] + segs[s] - 2 * half, half), :],
                send_sem=rs_ssem.at[s * nbits + k],
                recv_sem=rs_rsem.at[s * nbits + k],
                device_id=(me + (1 - 2 * beta) * (1 << bit),),
                device_id_type=MESH,
            )
            copy.start()
            flying[s] = copy

    def scatter_finish(group, k):
        for s in group:
            half = segs[s] >> (k + 1)
            flying[s].wait()
            keep = pl.ds(bases[s][k + 1], half)
            target = gbuf if k == nbits - 1 else acc
            target[keep, :] = acc[keep, :] + rbuf[pl.ds(starts[s] + segs[s] - 2 * half, half), :]

    def gather_start(group, k):
        for s in group:
            half = segs[s] >> (k + 1)
            bit = orders[s][k]
            part = pl.ds(bases[s][k + 1], half)
            copy = pltpu.make_async_remote_copy(
                src_ref=gbuf.at[part, :],
                dst_ref=gbuf.at[part, :],
                send_sem=ag_ssem.at[s * nbits + k],
                recv_sem=ag_rsem.at[s * nbits + k],
                device_id=(me + (1 - 2 * side(bit)) * (1 << bit),),
                device_id_type=MESH,
            )
            copy.start()
            flying[s] = copy

    def gather_finish(group, k):
        for s in group:
            flying[s].wait()

    work = [functools.partial(do_proj, j) for j in range(1, outputs // 256)]
    work += [functools.partial(do_ing, j) for j in range(width // 512)]
    rounds = 2 * nbits
    third = streams // 2
    groups = (range(third), range(third, streams))

    def begin(group, r):
        if r < nbits:
            scatter_start(group, r)
        elif r < rounds:
            gather_start(group, rounds - 1 - r)

    def end(group, r):
        if r < nbits:
            scatter_finish(group, r)
        else:
            gather_finish(group, rounds - 1 - r)

    def fill(slots):
        for _ in range(min(-(-len(work) // slots), len(work))):
            work.pop(0)()

    begin(groups[0], 0)
    begin(groups[1], 0)
    for r in range(rounds):
        for g in range(2):
            fill(2 * (rounds - r) - g)
            end(groups[g], r)
            begin(groups[g], r + 1)

    squares = jnp.zeros((8, 128), F32)
    for c in range(0, used, 128):
        piece = gbuf[pl.ds(c, 128), :]
        squares += jnp.sum((piece * piece).reshape(16, 8, 128), axis=0)
    norm = jnp.sqrt(jnp.sum(squares, axis=(0, 1), keepdims=True))
    limit = math.sqrt(width * ranks + ranks * outputs + width * experts)
    factor = jnp.minimum(1.0, limit / norm)
    for c in range(0, width, 128):
        gd_out[pl.ds(c, 128), :] = gbuf[pl.ds(c, 128), :].T * factor
        gg_out[:, pl.ds(c, 128)] = (
            gbuf[pl.ds(gate_at + c // 128 * experts, experts), :] * factor
        )
    for c in range(0, outputs, 128):
        gu_out[:, pl.ds(c, 128)] = gbuf[pl.ds(width + c, 128), :] * factor


def finish(rank, *refs):
    sources, stats, targets = refs[:5], refs[5], refs[6:11]
    load, ent, sem = refs[11:]
    copies = [
        pltpu.make_async_copy(sources[i], targets[i], sem.at[i]) for i in range(5)
    ]
    for copy in copies:
        copy.start()
    experts, ranks = load.shape[1], stats.shape[1]
    source = lax.broadcasted_iota(jnp.int32, (ranks, ranks), 0)
    target = lax.broadcasted_iota(jnp.int32, (ranks, ranks), 1)
    chosen = jnp.sum(
        jnp.where(source == target * rank, stats[0:1, :].T, 0.0), axis=0, keepdims=True
    )
    load[...] = chosen[:, :experts]
    ent[...] = stats[1:2, 0:1]
    for copy in copies:
        copy.wait()


def on_device(n, token_ids, tokens, frozen_weight, adapter_down, adapter_up, gate_weight, upstream):
    rows, width = tokens.shape
    experts = gate_weight.shape[1]
    ranks = adapter_down.shape[1]
    rank = ranks // experts
    outputs = frozen_weight.shape[1]
    nbits = n.bit_length() - 1
    head = list(range(1, nbits - 1))
    third = min(3, len(head))
    streams = 2 * third
    orders = [[0] + head[s:] + head[:s] + [nbits - 1] for s in range(third)] * 2
    used = width + outputs + width // 128 * experts
    unit = 8 * n
    units = -(-used // (third * unit))
    segs = [(units + 1) // 2 * unit] * third + [max(units // 2, 1) * unit] * third
    held = sum(segs)
    chunks = rows // min(256, rows)
    hbm = pl.BlockSpec(memory_space=pl.ANY)
    far = pl.BlockSpec(memory_space=pltpu.HBM)
    vmem = pl.BlockSpec(memory_space=pltpu.VMEM)
    dma = pltpu.SemaphoreType.DMA
    out = pl.pallas_call(
        functools.partial(kernel, n, experts, orders, segs),
        out_shape=(
            jax.ShapeDtypeStruct((rows, outputs), BF16),
            jax.ShapeDtypeStruct((rows, width), BF16),
            jax.ShapeDtypeStruct((width, ranks), F32),
            jax.ShapeDtypeStruct((ranks, outputs), F32),
            jax.ShapeDtypeStruct((experts, width), F32),
            jax.ShapeDtypeStruct((8, ranks), F32),
        ),
        in_specs=[vmem, far, far, far, far, vmem, far],
        out_specs=(vmem,) * 6,
        scratch_shapes=[
            pltpu.VMEM((rows, width), BF16),
            pltpu.VMEM((width, outputs), BF16),
            pltpu.VMEM((width, 2 * ranks), BF16),
            pltpu.VMEM((ranks, outputs), BF16),
            pltpu.VMEM((rows, outputs), BF16),
            pltpu.VMEM((rows, ranks), F32),
            pltpu.VMEM((rows, ranks), F32),
            pltpu.VMEM((rows, ranks), BF16),
            pltpu.VMEM((ranks, rows), BF16),
            pltpu.VMEM((rows, 2 * ranks), BF16),
            pltpu.VMEM((2 * ranks, rows), BF16),
            pltpu.VMEM((held, 128), F32),
            pltpu.VMEM((held, 128), F32),
            pltpu.VMEM((held, 128), F32),
            pltpu.VMEM((n - 1, 8, ranks), F32),
            pltpu.VMEM((8, ranks), F32),
            dma((4 + chunks,)),
            dma((n - 1,)),
            dma((n - 1,)),
            dma((streams * nbits,)),
            dma((streams * nbits,)),
            dma((streams * nbits,)),
            dma((streams * nbits,)),
        ],
        compiler_params=pltpu.CompilerParams(
            collective_id=0, vmem_limit_bytes=36 * 1024 * 1024
        ),
    )(
        token_ids.reshape(rows // 128, 128), tokens, frozen_weight, adapter_down, adapter_up,
        gate_weight.T, upstream,
    )
    proj, ing, down, up, gate, load, ent = pl.pallas_call(
        functools.partial(finish, rank),
        out_shape=tuple(jax.ShapeDtypeStruct(a.shape, a.dtype) for a in out[:5])
        + (jax.ShapeDtypeStruct((1, experts), F32), jax.ShapeDtypeStruct((1, 1), F32)),
        in_specs=[hbm] * 5 + [vmem],
        out_specs=(far,) * 5 + (vmem, vmem),
        scratch_shapes=[dma((5,))],
        compiler_params=pltpu.CompilerParams(vmem_limit_bytes=1024 * 1024),
    )(*out)
    return proj, ing, down, up, gate.T, load.reshape(experts), ent.reshape(())


def solution(mesh):
    placed = (P("dp"), P("dp", None), P(), P(), P(), P(), P("dp", None))
    return jax.shard_map(
        functools.partial(on_device, mesh.shape["dp"]),
        mesh=mesh,
        in_specs=placed,
        out_specs=(P("dp", None), P("dp", None), P(), P(), P(), P(), P()),
        check_vma=False,
    )
```
